32 devices in a mesh: wave: 16 (over z, x, core), lev: 2 (over y).
Axes of the slice: x: 2, y: 2, z: 4, core: 2. Of those that a mesh axis runs over, the one named last changes fastest.
Arguments:
- spectral: float32 [136, 256, 2562], P('lev', 'wave'), may hold values from -6 to 6
- to_modes: float32 [136, 136], replicated, may hold values from -3 to 3
- from_modes: float32 [136, 136], replicated, may hold values from -3 to 3
- depth: float32 [136], replicated, may hold values from 0.02 to 50
- owner: int32 [128], replicated, may hold values from 0 to 15, as said below
Outputs:
- solved: float32 [136, 128, 2562], P('lev', 'wave')
The draws below stay inside these ranges and needn't reach their ends.
Inputs may be any that keep to these rules, and one draw needn't show every extreme that they name: `owner`: group q holds the pairs q * 1 to q * 1 + 1 - 1; a device stores its groups in increasing q from its first slot on, 1 slots each, and leaves its other slots unused. The 8 groups with the same q // 8 have 8 different owners. A device owns at most 16 groups, and some device exactly that many.
All inputs are finite; a program needn't handle non-finite values.
Results may differ from the reference program's by a relative error of at most 0.000075.
Values sent between devices are 32-bit elements; how exact they have to be, the bound alone decides.
A program may use at most 128 MiB of HBM per device.

```python
import math
import jax
import jax.numpy as jnp
from jax import lax

NT = 1279
LEVELS = 136
KPAIR = 1
GROUPS = 8
PLEN = 1281
CAP = 16
PAIRS = 128
SLOTS = 256
NGROUPS = 128
N_WAVE = 16


def modes_matrix(key, salt):
    base = jax.random.fold_in(key, salt)
    first = jax.random.fold_in(base, 0)
    noise = jnp.clip(jax.random.normal(first, (LEVELS, LEVELS), jnp.float32), -4.0, 4.0)
    matrix = jnp.eye(LEVELS, dtype=jnp.float32) + 0.5 * noise / math.sqrt(LEVELS)
    return matrix


def draw_to_modes(key, part):
    return modes_matrix(key, 31)


def draw_from_modes(key, part):
    return modes_matrix(key, 47)


def draw_owner(key, part):
    first, second = jax.random.split(jax.random.fold_in(key, 11))
    half = N_WAVE // 2
    shifts = jax.random.randint(first, (half,), 0, GROUPS + 1).astype(jnp.int32)
    shifts = shifts.at[0].set(GROUPS)
    counts = jnp.concatenate([GROUPS + shifts, GROUPS - shifts])
    labels = jax.random.permutation(second, N_WAVE).astype(jnp.int32)
    bounds = jnp.cumsum(counts)
    positions = jnp.arange(NGROUPS, dtype=jnp.int32)
    runs = jnp.sum((positions[:, None] >= bounds[None, :]).astype(jnp.int32), axis=1)
    sequence = labels[runs]
    target = positions // GROUPS
    within = positions % GROUPS
    return sequence[within * N_WAVE + target].astype(jnp.int32)


def level_of(stream_key, dims, pieces, low, largest):
    factor_of, own = 1.0, jax.random.fold_in(stream_key, 6)
    for axis_at, parts in pieces:
        steps = jnp.exp(jax.random.uniform(jax.random.fold_in(own, axis_at), (parts,), jnp.float32, low / len(pieces), largest / len(pieces)))
        factor_of = factor_of * jnp.repeat(steps, dims[axis_at] // parts).reshape([-1 if axis == axis_at else 1 for axis in range(len(dims))])
    return factor_of


def scatter_about(own_key, shape, scale, bound, shards=(), kind=jnp.bfloat16):
    result = scale * jax.random.normal(own_key, shape, jnp.float32)
    if shards:
        result = result * level_of(own_key, shape, shards, -0.22, 0.18)
    return jnp.clip(result, -bound, bound).astype(kind)


def setup_inputs(seed: int = 0) -> dict:
    seeds = jax.random.split(jax.random.key(seed), 6)
    return {
        "spectral": scatter_about(seeds[0], (LEVELS, SLOTS, 2 * PLEN), 1.0, 6.0, ((0, 2), (1, 16)), jnp.float32),
        "to_modes": draw_to_modes(jax.random.fold_in(seeds[5], 71), 0),
        "from_modes": draw_from_modes(jax.random.fold_in(seeds[5], 71), 0),
        "depth": jnp.clip(jnp.exp(jax.random.uniform(seeds[3], (LEVELS,), jnp.float32, math.log(0.02), math.log(50.0))), 0.02, 50.0),
        "owner": draw_owner(jax.random.fold_in(seeds[5], 71), 0),
    }


def reference(spectral, to_modes, from_modes, depth, owner):
    numbers = jnp.arange(NGROUPS, dtype=jnp.int32)
    same = owner[:, None] == owner[None, :]
    rank = jnp.sum((same & (numbers[None, :] < numbers[:, None])).astype(jnp.int32), axis=1)
    first = owner * CAP + rank * KPAIR
    source = (first[:, None] + jnp.arange(KPAIR, dtype=jnp.int32)[None, :]).reshape(PAIRS).astype(jnp.int32)
    moved = jnp.take(spectral, source, axis=1)
    flat = moved.reshape(LEVELS, PAIRS * 2 * PLEN)
    pair = jnp.arange(PAIRS, dtype=jnp.int32)[:, None]
    column = jnp.arange(2 * PLEN, dtype=jnp.int32)[None, :]
    within = column % PLEN
    degree = jnp.where(within <= NT - pair, pair + within, within - 1)
    ratio = (degree * (degree + 1)).astype(jnp.float32) / float(NT * (NT + 1))
    ratio = ratio.reshape(PAIRS * 2 * PLEN)
    modes = jnp.dot(to_modes, flat, precision=lax.Precision.HIGHEST, preferred_element_type=jnp.float32)
    scaled = modes / (1.0 + depth[:, None] * ratio[None, :])
    solved = jnp.dot(from_modes, scaled, precision=lax.Precision.HIGHEST, preferred_element_type=jnp.float32)
    return solved.reshape(LEVELS, PAIRS, 2 * PLEN)
```

```python
import functools

import jax
import jax.numpy as jnp
from jax import lax
from jax.experimental import pallas as pl
from jax.experimental.pallas import tpu as pltpu
from jax.sharding import PartitionSpec as P

NT = 1279
KPAIR = 1
LANES = 128
TILES = 3
AHEAD = 2
MESH = pl.DeviceIdType.MESH


def flipped(index, mask, count):
    result = index * 0
    bit = 1
    while bit < count:
        own = lax.rem(lax.div(index, bit), 2)
        result = result + bit * ((1 - own) if mask & bit else own)
        bit *= 2
    return result


def halves(value):
    high = value.astype(jnp.bfloat16)
    low = (value - high.astype(jnp.float32)).astype(jnp.bfloat16)
    return high, low


def product(left_both, left_high, right, rows):
    high, low = halves(right)
    both = jnp.dot(left_both, high, preferred_element_type=jnp.float32)
    cross = jnp.dot(left_high, low, preferred_element_type=jnp.float32)
    return (both[rows:] + cross) + both[:rows]


def kernel(sizes, picks, places, spectral, last, to_modes, from_modes, depth, solved, *scratch):
    waves, levs, pairs, slots, levels, width, chunk, chunks = sizes
    received, rows_in = scratch[:chunks], scratch[chunks : 2 * chunks]
    sending, mine, theirs, to_both, from_both, staged = scratch[2 * chunks : 2 * chunks + 6]
    load_sem, send_sem, recv_sem, lev_send, lev_recv, out_sem = scratch[2 * chunks + 6 :]
    me = lax.axis_index("wave")
    lev = lax.axis_index("lev")
    modes_number = depth.shape[0]

    tiles = chunk // LANES

    def load(tile):
        whole = (tile + 1) * LANES <= width
        source = spectral.at[:, pl.ds(tile * LANES, LANES)] if whole else last
        return pltpu.make_async_copy(source, rows_in[tile // tiles].at[tile % tiles], load_sem.at[tile])

    for tile in range(chunks * tiles):
        load(tile).start()

    barrier = pltpu.get_barrier_semaphore()
    for mask in range(1, waves):
        pl.semaphore_signal(
            barrier, inc=1, device_id={"wave": flipped(me, mask, waves)}, device_id_type=MESH
        )
    for turn in range(1, levs):
        pl.semaphore_signal(
            barrier, inc=1, device_id={"lev": lax.rem(lev + turn, levs)}, device_id_type=MESH
        )

    for part in range(levs):
        high, low = halves(to_modes[part])
        to_both[part, :modes_number] = high
        to_both[part, modes_number:] = low
    high, low = halves(from_modes[...])
    from_both[0], from_both[1] = high, low
    pl.semaphore_wait(barrier, waves + levs - 2)

    def send(c):
        def pick(mask, target):
            slot = picks[flipped(me, mask, waves)]
            for tile in range(tiles):
                target[:, pl.ds(tile * LANES, LANES)] = rows_in[c][
                    tile, pl.ds(slot, levels, stride=slots), :
                ]

        for tile in range(c * tiles, (c + 1) * tiles):
            load(tile).wait()
        for mask in range(waves - 1, 0, -1):
            pick(mask, sending.at[c, mask - 1])
            pltpu.make_async_remote_copy(
                src_ref=sending.at[c, mask - 1],
                dst_ref=received[c].at[mask],
                send_sem=send_sem.at[c],
                recv_sem=recv_sem.at[c],
                device_id={"wave": flipped(me, mask, waves)},
                device_id_type=MESH,
            ).start()
        pick(0, received[c].at[0])

    def lev_copy(c, turn):
        return pltpu.make_async_remote_copy(
            src_ref=mine.at[c],
            dst_ref=theirs.at[c, turn - 1],
            send_sem=lev_send.at[c, turn - 1],
            recv_sem=lev_recv.at[c, turn - 1],
            device_id={"lev": lax.rem(lev + turn, levs)},
            device_id_type=MESH,
        )

    def out_copy(c):
        return pltpu.make_async_copy(
            staged.at[c], solved.at[:, :, pl.ds(c * chunk, chunk)], out_sem.at[c]
        )

    def gather(c):
        arrived = received[c].at[pl.ds(1, waves - 1)]
        pltpu.make_async_copy(arrived, arrived, recv_sem.at[c]).wait()

        @pl.loop(0, pairs)
        def _(pair):
            mine[c, pair] = received[c][places[pair]]

        for turn in range(1, levs):
            lev_copy(c, turn).start()

    def solve(c):
        for turn in range(1, levs):
            lev_copy(c, turn).wait_recv()
        column = lax.broadcasted_iota(jnp.int32, (1, chunk), 1) + c * chunk
        within = jnp.where(column >= NT + 2, column - (NT + 2), column)

        @pl.loop(0, pairs)
        def _(pair):
            wavenumber = me * pairs + pair
            degree = jnp.where(within <= NT - wavenumber, wavenumber + within, within - 1)
            ratio = (degree * (degree + 1)).astype(jnp.float32) / float(NT * (NT + 1))
            modes = None
            for turn in range(levs):
                source = lax.rem(lev + levs - turn, levs)
                block = mine[c, pair] if turn == 0 else theirs[c, turn - 1, pair]
                matrix = to_both.at[source]
                term = product(matrix[...], matrix[:modes_number], block, modes_number)
                modes = term if modes is None else modes + term
            scaled = modes / (1.0 + depth[...] * ratio)
            high, low = halves(scaled)
            from_high = from_both[0]
            result = jnp.dot(from_both[1], high, preferred_element_type=jnp.float32)
            result += jnp.dot(from_high, low, preferred_element_type=jnp.float32)
            result += jnp.dot(from_high, high, preferred_element_type=jnp.float32)
            staged[c, pair] = result

        out_copy(c).start()

    for c in range(min(AHEAD, chunks)):
        send(c)
    for c in range(chunks):
        if c + AHEAD < chunks:
            send(c + AHEAD)
        gather(c)
        if c >= 1:
            solve(c - 1)
    solve(chunks - 1)
    for c in range(chunks):
        pltpu.make_async_copy(sending.at[c], sending.at[c], send_sem.at[c]).wait()
        for turn in range(1, levs):
            lev_copy(c, turn).wait_send()
        out_copy(c).wait()


def per_device(spectral, to_modes, from_modes, depth, owner):
    waves, levs = lax.axis_size("wave"), lax.axis_size("lev")
    levels, slots, width = spectral.shape
    groups = owner.shape[0] // waves
    pairs = groups * KPAIR
    modes_number = depth.shape[0]
    own_index, lev_index = lax.axis_index("wave"), lax.axis_index("lev")
    numbers = jnp.arange(owner.shape[0], dtype=jnp.int32)
    mine = owner == own_index
    before = (numbers[:, None] > numbers[None, :]) & mine[None, :]
    rank = jnp.sum(before.astype(jnp.int32), axis=1)
    picks = jnp.sum(jnp.where(mine, rank, 0).reshape(waves, groups), axis=1)
    places = lax.dynamic_slice_in_dim(owner, own_index * groups, groups) ^ own_index
    chunk = TILES * LANES
    chunks = pl.cdiv(width, chunk)
    sizes = (waves, levs, pairs, slots, levels, width, chunk, chunks)
    rows = spectral.reshape(levels * slots, width)
    full = width // LANES * LANES
    last = jnp.pad(rows[:, full:], ((0, 0), (0, full + LANES - width)))
    by_lev = to_modes.reshape(modes_number, levs, levels).transpose(1, 0, 2)
    own_rows = lax.dynamic_slice_in_dim(from_modes, lev_index * levels, levels)
    vmem, smem, anywhere = (
        pl.BlockSpec(memory_space=space) for space in (pltpu.VMEM, pltpu.SMEM, pl.ANY)
    )
    dma = pltpu.SemaphoreType.DMA
    f32, bf16 = jnp.float32, jnp.bfloat16
    solved = pl.pallas_call(
        functools.partial(kernel, sizes),
        out_shape=jax.ShapeDtypeStruct((pairs, levels, chunks * chunk), f32),
        in_specs=[smem, smem, anywhere, anywhere, vmem, vmem, vmem],
        out_specs=anywhere,
        scratch_shapes=[pltpu.VMEM((waves, levels, chunk), f32) for _ in range(chunks)]
        + [pltpu.VMEM((TILES, levels * slots, LANES), f32) for _ in range(chunks)]
        + [
            pltpu.VMEM((chunks, waves - 1, levels, chunk), f32),
            pltpu.VMEM((chunks, pairs, levels, chunk), f32),
            pltpu.VMEM((chunks, levs - 1, pairs, levels, chunk), f32),
            pltpu.VMEM((levs, 2 * modes_number, levels), bf16),
            pltpu.VMEM((2, levels, modes_number), bf16),
            pltpu.VMEM((chunks, pairs, levels, chunk), f32),
            dma((chunks * TILES,)),
            dma((chunks,)),
            dma((chunks,)),
            dma((chunks, levs - 1)),
            dma((chunks, levs - 1)),
            dma((chunks,)),
        ],
        compiler_params=pltpu.CompilerParams(
            collective_id=0, has_side_effects=True, vmem_limit_bytes=67043328
        ),
    )(picks, places, rows, last, by_lev, own_rows, depth[:, None])
    return solved[:, :, :width].transpose(1, 0, 2)


def solution(mesh):
    placed = (P("lev", "wave", None), P(), P(), P(), P())
    return jax.shard_map(
        per_device, mesh=mesh, in_specs=placed, out_specs=P("lev", "wave", None), check_vma=False
    )
```

```python
import functools

import jax
import jax.numpy as jnp
from jax import lax
from jax.experimental import pallas as pl
from jax.experimental.pallas import tpu as pltpu
from jax.sharding import PartitionSpec as P

NT = 1279
KPAIR = 1
LANES = 128
TILES = 3
AHEAD = 2
MESH = pl.DeviceIdType.MESH


def flipped(index, mask, count):
    result = index * 0
    bit = 1
    while bit < count:
        own = lax.rem(lax.div(index, bit), 2)
        result = result + bit * ((1 - own) if mask & bit else own)
        bit *= 2
    return result


def halves(value):
    high = value.astype(jnp.bfloat16)
    low = (value - high.astype(jnp.float32)).astype(jnp.bfloat16)
    return high, low


def product(left_both, left_high, right, rows):
    high, low = halves(right)
    both = jnp.dot(left_both, high, preferred_element_type=jnp.float32)
    cross = jnp.dot(left_high, low, preferred_element_type=jnp.float32)
    return (both[rows:] + cross) + both[:rows]


def kernel(sizes, picks, places, spectral, last, to_modes, from_modes, depth, solved, *scratch):
    waves, levs, pairs, slots, levels, width, parts, packs, rest = sizes
    chunks = len(parts)
    received, rows_in, sending, mine, theirs, staged = (
        scratch[kind * chunks : (kind + 1) * chunks] for kind in range(6)
    )
    rows_last, tail_sent, tail_got, tail_mine, tail_theirs = scratch[6 * chunks : 6 * chunks + 5]
    to_both, from_both, load_sem, send_sem, recv_sem, lev_send, lev_recv, out_sem = scratch[
        6 * chunks + 5 :
    ]
    me = lax.axis_index("wave")
    lev = lax.axis_index("lev")
    modes_number = depth.shape[0]
    firsts = [sum(parts[:c]) for c in range(chunks)]
    final = chunks - 1

    def load(c, tile):
        number = firsts[c] + tile
        if number < sum(parts):
            source = spectral.at[:, pl.ds(number * LANES, LANES)]
            return pltpu.make_async_copy(source, rows_in[c].at[tile], load_sem.at[number])
        target = rows_last.at[pl.ds(0, levels * slots)]
        return pltpu.make_async_copy(last, target, load_sem.at[number])

    def width_of(c):
        return parts[c] + (1 if c == final else 0)

    for c in range(chunks):
        for tile in range(width_of(c)):
            load(c, tile).start()

    barrier = pltpu.get_barrier_semaphore()
    for mask in range(1, waves):
        pl.semaphore_signal(
            barrier, inc=1, device_id={"wave": flipped(me, mask, waves)}, device_id_type=MESH
        )
    for turn in range(1, levs):
        pl.semaphore_signal(
            barrier, inc=1, device_id={"lev": lax.rem(lev + turn, levs)}, device_id_type=MESH
        )

    for part in range(levs):
        high, low = halves(to_modes[part])
        to_both[part, :modes_number] = high
        to_both[part, modes_number:] = low
    high, low = halves(from_modes[...])
    from_both[0], from_both[1] = high, low
    pl.semaphore_wait(barrier, waves + levs - 2)

    def packed(slot):
        lane = lax.broadcasted_iota(jnp.int32, (8, LANES), 1)
        total = rows_last[pl.ds(slot, 8, stride=slots), :]
        for k in range(1, packs):
            block = rows_last[pl.ds(8 * k * slots + slot, 8, stride=slots), :]
            total = jnp.where(lane >= k * rest, pltpu.roll(block, k * rest, 1), total)
        return total

    def unpacked(block):
        pieces = [block] + [pltpu.roll(block, LANES - k * rest, 1) for k in range(1, packs)]
        return jnp.concatenate(pieces, axis=0)[:levels]

    def send(c):
        for tile in range(width_of(c)):
            load(c, tile).wait()

        def pick(mask, target):
            slot = picks[flipped(me, mask, waves)]
            for tile in range(parts[c]):
                target[:, pl.ds(tile * LANES, LANES)] = rows_in[c][
                    tile, pl.ds(slot, levels, stride=slots), :
                ]

        def push(mask, source, target, number):
            pltpu.make_async_remote_copy(
                src_ref=source.at[mask - 1],
                dst_ref=target.at[mask],
                send_sem=send_sem.at[number],
                recv_sem=recv_sem.at[number],
                device_id={"wave": flipped(me, mask, waves)},
                device_id_type=MESH,
            ).start()

        if c == final:
            for mask in range(waves - 1, 0, -1):
                tail_sent[mask - 1] = packed(picks[flipped(me, mask, waves)])
                push(mask, tail_sent, tail_got, chunks)
            tail_got[0] = packed(picks[me])
        for mask in range(waves - 1, 0, -1):
            pick(mask, sending[c].at[mask - 1])
            push(mask, sending[c], received[c], c)
        pick(0, received[c].at[0])

    def lev_copy(c, turn):
        source, target = (tail_mine, tail_theirs) if c == chunks else (mine[c], theirs[c])
        return pltpu.make_async_remote_copy(
            src_ref=source,
            dst_ref=target.at[turn - 1],
            send_sem=lev_send.at[c, turn - 1],
            recv_sem=lev_recv.at[c, turn - 1],
            device_id={"lev": lax.rem(lev + turn, levs)},
            device_id_type=MESH,
        )

    def out_copy(c, tile):
        number = firsts[c] + tile
        columns = solved.at[:, pl.ds(number * LANES, LANES)]
        return pltpu.make_async_copy(staged[c].at[tile], columns, out_sem.at[number])

    def gather(c):
        if c == final:
            arrived = tail_got.at[pl.ds(1, waves - 1)]
            pltpu.make_async_copy(arrived, arrived, recv_sem.at[chunks]).wait()
            for pair in range(pairs):
                tail_mine[pair] = tail_got[places[pair]]
            for turn in range(1, levs):
                lev_copy(chunks, turn).start()
        arrived = received[c].at[pl.ds(1, waves - 1)]
        pltpu.make_async_copy(arrived, arrived, recv_sem.at[c]).wait()

        @pl.loop(0, pairs)
        def _(pair):
            mine[c][pair] = received[c][places[pair]]

        for turn in range(1, levs):
            lev_copy(c, turn).start()

    def solve(c):
        for turn in range(1, levs):
            lev_copy(c, turn).wait_recv()
            if c == final:
                lev_copy(chunks, turn).wait_recv()
        size = width_of(c) * LANES
        column = lax.broadcasted_iota(jnp.int32, (1, size), 1) + firsts[c] * LANES
        within = jnp.where(column >= width // 2, column - width // 2, column)

        @pl.loop(0, pairs)
        def _(pair):
            wavenumber = me * pairs + pair
            degree = jnp.where(within <= NT - wavenumber, wavenumber + within, within - 1)
            ratio = (degree * (degree + 1)).astype(jnp.float32) / float(NT * (NT + 1))
            modes = None
            for turn in range(levs):
                source = lax.rem(lev + levs - turn, levs)
                block = mine[c][pair] if turn == 0 else theirs[c][turn - 1, pair]
                if c == final:
                    tail = tail_mine[pair] if turn == 0 else tail_theirs[turn - 1, pair]
                    block = jnp.concatenate([block, unpacked(tail)], axis=1)
                matrix = to_both.at[source]
                term = product(matrix[...], matrix[:modes_number], block, modes_number)
                modes = term if modes is None else modes + term
            scaled = modes / (1.0 + depth[...] * ratio)
            high, low = halves(scaled)
            from_high = from_both[0]
            result = jnp.dot(from_both[1], high, preferred_element_type=jnp.float32)
            result += jnp.dot(from_high, low, preferred_element_type=jnp.float32)
            result += jnp.dot(from_high, high, preferred_element_type=jnp.float32)
            for tile in range(width_of(c)):
                staged[c][tile, pl.ds(pair, levels, stride=pairs), :] = result[
                    :, tile * LANES : (tile + 1) * LANES
                ]

        for tile in range(width_of(c)):
            out_copy(c, tile).start()

    for c in range(min(AHEAD, chunks)):
        send(c)
    for c in range(chunks):
        if c + AHEAD < chunks:
            send(c + AHEAD)
        gather(c)
        if c >= 1:
            solve(c - 1)
    solve(final)
    for c in range(chunks + 1):
        sent = tail_sent if c == chunks else sending[c]
        pltpu.make_async_copy(sent, sent, send_sem.at[c]).wait()
        for turn in range(1, levs):
            lev_copy(c, turn).wait_send()
    for c in range(chunks):
        for tile in range(width_of(c)):
            out_copy(c, tile).wait()


def per_device(spectral, to_modes, from_modes, depth, owner):
    waves, levs = lax.axis_size("wave"), lax.axis_size("lev")
    levels, slots, width = spectral.shape
    groups = owner.shape[0] // waves
    pairs = groups * KPAIR
    modes_number = depth.shape[0]
    own_index, lev_index = lax.axis_index("wave"), lax.axis_index("lev")
    numbers = jnp.arange(owner.shape[0], dtype=jnp.int32)
    mine = owner == own_index
    before = (numbers[:, None] > numbers[None, :]) & mine[None, :]
    rank = jnp.sum(before.astype(jnp.int32), axis=1)
    picks = jnp.sum(jnp.where(mine, rank, 0).reshape(waves, groups), axis=1)
    places = lax.dynamic_slice_in_dim(owner, own_index * groups, groups) ^ own_index
    whole, rest = width // LANES, width % LANES
    packs = pl.cdiv(levels, 8)
    assert 0 < rest and packs * rest <= LANES
    parts = (TILES,) * (whole // TILES) + ((whole % TILES,) if whole % TILES else ())
    chunks = len(parts)
    sizes = (waves, levs, pairs, slots, levels, width, parts, packs, rest)
    rows = spectral.reshape(levels * slots, width)
    last = jnp.pad(rows[:, whole * LANES :], ((0, 0), (0, LANES - rest)))
    by_lev = to_modes.reshape(modes_number, levs, levels).transpose(1, 0, 2)
    own_rows = lax.dynamic_slice_in_dim(from_modes, lev_index * levels, levels)
    vmem, smem, anywhere = (
        pl.BlockSpec(memory_space=space) for space in (pltpu.VMEM, pltpu.SMEM, pl.ANY)
    )
    dma = pltpu.SemaphoreType.DMA
    f32, bf16 = jnp.float32, jnp.bfloat16
    widths = [tiles * LANES for tiles in parts]
    staged_tiles = parts[:-1] + (parts[-1] + 1,)
    solved = pl.pallas_call(
        functools.partial(kernel, sizes),
        out_shape=jax.ShapeDtypeStruct((levels * pairs, (whole + 1) * LANES), f32),
        in_specs=[smem, smem, anywhere, anywhere, vmem, vmem, vmem],
        out_specs=anywhere,
        scratch_shapes=[pltpu.VMEM((waves, levels, size), f32) for size in widths]
        + [pltpu.VMEM((tiles, levels * slots, LANES), f32) for tiles in parts]
        + [pltpu.VMEM((waves - 1, levels, size), f32) for size in widths]
        + [pltpu.VMEM((pairs, levels, size), f32) for size in widths]
        + [pltpu.VMEM((levs - 1, pairs, levels, size), f32) for size in widths]
        + [pltpu.VMEM((tiles, levels * pairs, LANES), f32) for tiles in staged_tiles]
        + [
            pltpu.VMEM((8 * packs * slots, LANES), f32),
            pltpu.VMEM((waves - 1, 8, LANES), f32),
            pltpu.VMEM((waves, 8, LANES), f32),
            pltpu.VMEM((pairs, 8, LANES), f32),
            pltpu.VMEM((levs - 1, pairs, 8, LANES), f32),
            pltpu.VMEM((levs, 2 * modes_number, levels), bf16),
            pltpu.VMEM((2, levels, modes_number), bf16),
            dma((whole + 1,)),
            dma((chunks + 1,)),
            dma((chunks + 1,)),
            dma((chunks + 1, levs - 1)),
            dma((chunks + 1, levs - 1)),
            dma((whole + 1,)),
        ],
        compiler_params=pltpu.CompilerParams(
            collective_id=0, has_side_effects=True, vmem_limit_bytes=67043328
        ),
    )(picks, places, rows, last, by_lev, own_rows, depth[:, None])
    return solved.reshape(levels, pairs, (whole + 1) * LANES)[:, :, :width]


def solution(mesh):
    placed = (P("lev", "wave", None), P(), P(), P(), P())
    return jax.shard_map(
        per_device, mesh=mesh, in_specs=placed, out_specs=P("lev", "wave", None), check_vma=False
    )
```
